32 devices in a mesh: groups: 2 (over x), seq: 16 (over z, y, core).
Axes of the slice: x: 2, y: 2, z: 4, core: 2. Of those that a mesh axis runs over, the one named last changes fastest.
Arguments:
- video_qkv: bfloat16 [8, 16, 3, 3072, 128], P('groups', None, None, 'seq'), parts along dimension 0, may hold values from -9 to 9
- video_cross: bfloat16 [8, 16, 3, 3072, 128], P('groups', None, None, 'seq'), parts along dimension 0, may hold values from -9 to 9
- audio_qkv: bfloat16 [8, 16, 3, 768, 128], P('groups', None, None, 'seq'), parts along dimension 0, may hold values from -9 to 9
- audio_cross: bfloat16 [8, 16, 3, 768, 128], P('groups', None, None, 'seq'), parts along dimension 0, may hold values from -9 to 9
- lengths: int32 [2, 8], P(None, 'groups'), parts along dimension 1, may hold values from 384 to 3072, as said below
- timestep: int32 [2], P('groups'), parts along dimension 0, may hold values from 0 to 49
- gate_table: float32 [50, 4, 16, 128], replicated, may hold values from -4 to 4
Outputs:
- video_out: bfloat16 [8, 16, 3072, 128], P('groups', None, 'seq'), parts along dimension 0
- audio_out: bfloat16 [8, 16, 768, 128], P('groups', None, 'seq'), parts along dimension 0
The draws below stay inside these ranges and needn't reach their ends.
There are 2 independent parts, one for each index of `groups`. The reference program is written for one: setup_inputs(seed, part) draws one part's arguments, and reference() takes and returns one part's arrays. A program takes and returns all parts, laid end to end along the dimension named above; an argument that names none is the same for every part. Nothing has to cross between parts.
Inputs may be any that keep to these rules, and one draw needn't show every extreme that they name: `lengths`: row 0 holds each clip's valid video token count, row 1 its valid audio token count; every count is at least half of its tower's length (3072 or 768), and in every draw some clip has all 3072 video tokens and some clip all 768 audio tokens valid.
All inputs are finite; a program needn't handle non-finite values.
Results may differ from the reference program's by a relative error of at most 0.0085.
Values may be sent and summed in bfloat16 or wider, within the bound.
A program may use at most 128 MiB of HBM per device.

```python
import math
import jax
import jax.numpy as jnp
from jax import lax

HEADS = 16
HEADDIM = 128
SEQS = 4
LV = 3072
LA = 768
STEPS = 50


def noise_block(key, length):
    subkeys = jax.random.split(key, 3)
    block_shape = (SEQS, HEADS, length, HEADDIM)
    query_part = jnp.clip(1.5 * jax.random.normal(subkeys[0], block_shape, jnp.float32), -9.0, 9.0)
    key_part = jnp.clip(1.5 * jax.random.normal(subkeys[1], block_shape, jnp.float32), -9.0, 9.0)
    value_part = jnp.clip(jax.random.normal(subkeys[2], block_shape, jnp.float32), -9.0, 9.0)
    return (query_part, key_part, value_part)


def stacked(query_part, key_part, value_part):
    return jnp.stack([query_part, key_part, value_part], axis=2).astype(jnp.bfloat16)


def draw_video_qkv(key, part):
    query_part, key_part, value_part = noise_block(jax.random.fold_in(key, 11), LV)
    return stacked(query_part, key_part, value_part)


def draw_audio_qkv(key, part):
    query_part, key_part, value_part = noise_block(jax.random.fold_in(key, 13), LA)
    return stacked(query_part, key_part, value_part)


def draw_video_cross(key, part):
    query_part, key_part, value_part = noise_block(jax.random.fold_in(key, 12), LV)
    return stacked(query_part, key_part, value_part)


def draw_audio_cross(key, part):
    query_part, key_part, value_part = noise_block(jax.random.fold_in(key, 14), LA)
    return stacked(query_part, key_part, value_part)


def draw_lengths(key, part):
    subkeys = jax.random.split(jax.random.fold_in(key, 31), 4)
    video_count = jax.random.randint(subkeys[0], (SEQS,), LV // 2, LV + 1)
    audio_count = jax.random.randint(subkeys[1], (SEQS,), LA // 2, LA + 1)
    full_video = jax.random.randint(subkeys[2], (), 0, SEQS)
    full_audio = jax.random.randint(subkeys[3], (), 0, SEQS)
    clip_index = jnp.arange(SEQS)
    video_count = jnp.where(clip_index == full_video, LV, video_count)
    audio_count = jnp.where(clip_index == full_audio, LA, audio_count)
    return jnp.stack([video_count, audio_count]).astype(jnp.int32)


def noise(own_key, extent, spread, bound, held_as=jnp.bfloat16):
    return jnp.clip(spread * jax.random.normal(own_key, extent, jnp.float32), -bound, bound).astype(held_as)


def setup_inputs(seed: int = 0, part: int = 0) -> dict:
    streams_of = jax.random.split(jax.random.key(seed), 8)
    part_splits = jax.random.split(jax.random.fold_in(streams_of[7], part), 8)
    return {
        "video_qkv": draw_video_qkv(jax.random.fold_in(jax.random.fold_in(streams_of[7], part), 71), part),
        "video_cross": draw_video_cross(jax.random.fold_in(jax.random.fold_in(streams_of[7], part), 71), part),
        "audio_qkv": draw_audio_qkv(jax.random.fold_in(jax.random.fold_in(streams_of[7], part), 71), part),
        "audio_cross": draw_audio_cross(jax.random.fold_in(jax.random.fold_in(streams_of[7], part), 71), part),
        "lengths": draw_lengths(jax.random.fold_in(jax.random.fold_in(streams_of[7], part), 71), part),
        "timestep": jax.random.randint(part_splits[5], (1,), 0, STEPS).astype(jnp.int32),
        "gate_table": noise(streams_of[6], (STEPS, 4, HEADS, HEADDIM), 1.0, 4.0, jnp.float32),
    }


def attend(queries, key_rows, values, keep_len):
    row_count = queries.shape[0]
    block_rows = row_count if row_count <= 1024 else math.gcd(row_count, 1024)
    score_scale = 1.0 / math.sqrt(queries.shape[1])
    columns = jnp.arange(key_rows.shape[0], dtype=jnp.int32)
    visible = columns[None, :] < keep_len
    blocks = queries.reshape(row_count // block_rows, block_rows, queries.shape[1])

    def one_block(query_block):
        scores = lax.dot_general(query_block, key_rows, (((1,), (1,)), ((), ())), preferred_element_type=jnp.float32) * score_scale
        scores = jnp.where(visible, scores, -1e+30)
        row_max = lax.optimization_barrier(jnp.max(scores, axis=1, keepdims=True))
        weights = jnp.exp(scores - row_max)
        row_total = lax.optimization_barrier(jnp.sum(weights, axis=1, keepdims=True))
        shares = (weights / row_total).astype(jnp.bfloat16)
        return jnp.dot(shares, values, preferred_element_type=jnp.float32).astype(jnp.bfloat16)
    return lax.map(one_block, blocks).reshape(row_count, queries.shape[1])

def pair_outputs(bundle):
    video_set, video_far, audio_set, audio_far, video_len, audio_len = bundle
    self_video = attend(video_set[0], video_set[1], video_set[2], video_len)
    cross_video = attend(video_far[0], audio_far[1], audio_far[2], audio_len)
    self_audio = attend(audio_set[0], audio_set[1], audio_set[2], audio_len)
    cross_audio = attend(audio_far[0], video_far[1], video_far[2], video_len)
    return (self_video, cross_video, self_audio, cross_audio)

def combine(self_part, cross_part, gate_self, gate_cross, clip_count):
    head_count = gate_self.shape[0]
    shaped = (clip_count, head_count) + self_part.shape[1:]
    mixed_sum = gate_self[None, :, None, :] * self_part.reshape(shaped).astype(jnp.float32) + gate_cross[None, :, None, :] * cross_part.reshape(shaped).astype(jnp.float32)
    return mixed_sum.astype(jnp.bfloat16)

def reference(video_qkv, video_cross, audio_qkv, audio_cross, lengths, timestep, gate_table):
    clip_count, head_count = (video_qkv.shape[0], video_qkv.shape[1])
    pair_count = clip_count * head_count
    step_ids = jnp.arange(gate_table.shape[0], dtype=jnp.int32)
    gate_rows = lax.optimization_barrier(jnp.sum(jnp.where((step_ids == timestep[0])[:, None, None, None], gate_table, 0.0), axis=0))
    clip_ids = jnp.arange(pair_count, dtype=jnp.int32) // head_count
    video_lens = lengths[0][clip_ids].astype(jnp.int32)
    audio_lens = lengths[1][clip_ids].astype(jnp.int32)

    def to_pairs(tensor):
        return tensor.reshape((pair_count,) + tensor.shape[2:])
    self_video, cross_video, self_audio, cross_audio = lax.map(pair_outputs, (to_pairs(video_qkv), to_pairs(video_cross), to_pairs(audio_qkv), to_pairs(audio_cross), video_lens, audio_lens))
    video_out = combine(self_video, cross_video, gate_rows[0], gate_rows[1], clip_count)
    audio_out = combine(self_audio, cross_audio, gate_rows[2], gate_rows[3], clip_count)
    return (video_out, audio_out)
```

```python
import functools
import math

import jax
import jax.numpy as jnp
from jax import lax
from jax.experimental import pallas as pl
from jax.experimental.pallas import tpu as pltpu
from jax.sharding import PartitionSpec as P

ROW_TILE = 16
MESH_ID = pl.DeviceIdType.MESH


def attend(queries, key_rows, values, bias, score_scale):
    scores = lax.dot_general(
        queries, key_rows, (((1,), (1,)), ((), ())), preferred_element_type=jnp.float32
    )
    scores = scores * score_scale + bias
    row_max = jnp.max(scores, axis=1, keepdims=True)
    weights = jnp.exp2(scores - row_max)
    row_total = jnp.sum(weights, axis=1, keepdims=True)
    mixed = jnp.dot(weights.astype(jnp.bfloat16), values, preferred_element_type=jnp.float32)
    return (mixed / row_total).astype(jnp.bfloat16).astype(jnp.float32)


def key_bias(total, padded, rows, keep_len):
    column = lax.broadcasted_iota(jnp.int32, (1, total), 1)
    if padded == rows:
        visible = column < keep_len
    else:
        row = column % padded
        visible = (row < rows) & ((column // padded) * rows + row < keep_len)
    return jnp.where(visible, 0.0, -1e30)


def kernel(
    group, clips, heads, local, rows_v, rows_a, pad_a, size,
    vq_hbm, vc_hbm, aq_hbm, ac_hbm, len_ref, gate_ref,
    vout_hbm, aout_hbm,
    vq, vc, aq, ac, vres, ares,
    in_send, in_recv, out_send, out_recv,
):
    me = lax.axis_index("seq")
    total_v, total_a = group * rows_v, group * pad_a
    streams = (
        (vq_hbm, vq, rows_v),
        (aq_hbm, aq, pad_a),
        (vc_hbm, vc, rows_v),
        (ac_hbm, ac, pad_a),
    )

    def clip_head(device, j):
        pair = device * local + j
        return pair // heads, pair % heads

    barrier = pltpu.get_barrier_semaphore()

    def greet(t, carry):
        pl.semaphore_signal(
            barrier, inc=1, device_id={"seq": (me + t) % group}, device_id_type=MESH_ID
        )
        return carry

    lax.fori_loop(1, group, greet, 0)
    pl.semaphore_wait(barrier, group - 1)

    def send_inputs(j):
        def to_one(t, carry):
            there = (me + t) % group
            clip, head = clip_head(there, j)
            for k, (source, buffer, rows) in enumerate(streams):
                pltpu.make_async_remote_copy(
                    src_ref=source.at[clip, head],
                    dst_ref=buffer.at[j, :, pl.ds(pl.multiple_of(me * rows, ROW_TILE), rows), :],
                    send_sem=in_send.at[k, j],
                    recv_sem=in_recv.at[k, j],
                    device_id={"seq": there},
                    device_id_type=MESH_ID,
                ).start()
            return carry

        clip, head = clip_head(me, j)
        for k, (source, buffer, rows) in enumerate(streams):
            pltpu.make_async_copy(
                source.at[clip, head],
                buffer.at[j, :, pl.ds(pl.multiple_of(me * rows, ROW_TILE), rows), :],
                in_recv.at[k, j],
            ).start()
        lax.fori_loop(1, group, to_one, 0)

    results = ((vout_hbm, vres, rows_v), (aout_hbm, ares, pad_a))

    def send_outputs(j, k):
        target, buffer, rows = results[k]
        clip, head = clip_head(me, j)

        def to_one(t, carry):
            there = (me + t) % group
            pltpu.make_async_remote_copy(
                src_ref=buffer.at[j, pl.ds(pl.multiple_of(there * rows, ROW_TILE), rows), :],
                dst_ref=target.at[clip, head],
                send_sem=out_send.at[k, j],
                recv_sem=out_recv.at[k],
                device_id={"seq": there},
                device_id_type=MESH_ID,
            ).start()
            return carry

        pltpu.make_async_copy(
            buffer.at[j, pl.ds(pl.multiple_of(me * rows, ROW_TILE), rows), :],
            target.at[clip, head],
            out_recv.at[k],
        ).start()
        lax.fori_loop(1, group, to_one, 0)

    def wait_bytes(ref, sem):
        pltpu.make_async_copy(ref, ref, sem).wait()

    score_scale = math.log2(math.e) / math.sqrt(size)
    block_v, block_a = math.gcd(total_v, 256), math.gcd(total_a, 256)

    send_inputs(0)
    if local > 1:
        send_inputs(1)

    def one_pair(j, carry):
        for k, (_, buffer, _) in enumerate(streams):
            wait_bytes(buffer.at[j], in_recv.at[k, j])

        @pl.when(j + 2 < local)
        def _():
            send_inputs(j + 2)

        clip, head = clip_head(me, j)
        bias_v = key_bias(total_v, rows_v, rows_v, len_ref[0, clip])
        bias_a = key_bias(total_a, pad_a, rows_a, len_ref[1, clip])
        gates = [gate_ref[k, pl.ds(head, 1), :] for k in range(4)]

        def video_block(i, c):
            rows = pl.ds(pl.multiple_of(i * block_v, block_v), block_v)
            near = attend(vq[j, 0, rows, :], vq[j, 1], vq[j, 2], bias_v, score_scale)
            far = attend(vc[j, 0, rows, :], ac[j, 1], ac[j, 2], bias_a, score_scale)
            vres[j, rows, :] = (gates[0] * near + gates[1] * far).astype(jnp.bfloat16)
            return c

        lax.fori_loop(0, total_v // block_v, video_block, 0)
        send_outputs(j, 0)

        def audio_block(i, c):
            rows = pl.ds(pl.multiple_of(i * block_a, block_a), block_a)
            near = attend(aq[j, 0, rows, :], aq[j, 1], aq[j, 2], bias_a, score_scale)
            far = attend(ac[j, 0, rows, :], vc[j, 1], vc[j, 2], bias_v, score_scale)
            ares[j, rows, :] = (gates[2] * near + gates[3] * far).astype(jnp.bfloat16)
            return c

        lax.fori_loop(0, total_a // block_a, audio_block, 0)
        send_outputs(j, 1)
        return carry

    lax.fori_loop(0, local, one_pair, 0)

    def drain(j, carry):
        for k, (_, buffer, rows) in enumerate(streams):
            wait_bytes(buffer.at[j, :, pl.ds(0, (group - 1) * rows), :], in_send.at[k, j])
        for k, (_, buffer, rows) in enumerate(results):
            wait_bytes(buffer.at[j, pl.ds(0, (group - 1) * rows), :], out_send.at[k, j])
        return carry

    lax.fori_loop(0, local, drain, 0)
    for k, (target, _, _) in enumerate(results):
        wait_bytes(target, out_recv.at[k])


def on_device(video_qkv, video_cross, audio_qkv, audio_cross, lengths, timestep, gate_table):
    group = lax.axis_size("seq")
    clips, heads, _, rows_v, size = video_qkv.shape
    rows_a = audio_qkv.shape[3]
    local = clips * heads // group
    pad_a = -(-rows_a // ROW_TILE) * ROW_TILE
    if pad_a != rows_a:
        extra = ((0, 0), (0, 0), (0, 0), (0, pad_a - rows_a), (0, 0))
        audio_qkv, audio_cross = jnp.pad(audio_qkv, extra), jnp.pad(audio_cross, extra)
    gate_rows = lax.dynamic_index_in_dim(gate_table, timestep[0], 0, keepdims=False)
    total_v, total_a = group * rows_v, group * pad_a
    any_spec = pl.BlockSpec(memory_space=pl.ANY)
    dtype = video_qkv.dtype
    video_out, audio_out = pl.pallas_call(
        functools.partial(kernel, group, clips, heads, local, rows_v, rows_a, pad_a, size),
        out_shape=(
            jax.ShapeDtypeStruct((clips, heads, rows_v, size), dtype),
            jax.ShapeDtypeStruct((clips, heads, pad_a, size), dtype),
        ),
        in_specs=[any_spec] * 4
        + [pl.BlockSpec(memory_space=pltpu.SMEM), pl.BlockSpec(memory_space=pltpu.VMEM)],
        out_specs=(any_spec, any_spec),
        scratch_shapes=[
            pltpu.VMEM((local, 3, total_v, size), dtype),
            pltpu.VMEM((local, 3, total_v, size), dtype),
            pltpu.VMEM((local, 3, total_a, size), dtype),
            pltpu.VMEM((local, 3, total_a, size), dtype),
            pltpu.VMEM((local, total_v, size), dtype),
            pltpu.VMEM((local, total_a, size), dtype),
            pltpu.SemaphoreType.DMA((4, local)),
            pltpu.SemaphoreType.DMA((4, local)),
            pltpu.SemaphoreType.DMA((2, local)),
            pltpu.SemaphoreType.DMA((2,)),
        ],
        compiler_params=pltpu.CompilerParams(
            collective_id=0, has_side_effects=True, vmem_limit_bytes=60000 * 1024
        ),
    )(video_qkv, video_cross, audio_qkv, audio_cross, lengths, gate_rows)
    return (video_out, audio_out[:, :, :rows_a])


def solution(mesh):
    in_specs = (
        P("groups", None, None, "seq", None),
        P("groups", None, None, "seq", None),
        P("groups", None, None, "seq", None),
        P("groups", None, None, "seq", None),
        P(None, "groups"),
        P("groups"),
        P(),
    )
    out_specs = (P("groups", None, "seq", None), P("groups", None, "seq", None))
    return jax.shard_map(
        on_device, mesh=mesh, in_specs=in_specs, out_specs=out_specs, check_vma=False
    )
```
